32 devices in a mesh: atoms: 16 (over z, y, x), chan: 2 (over core).
Axes of the slice: x: 2, y: 2, z: 4, core: 2. Of those that a mesh axis runs over, the one named last changes fastest.
Arguments:
- features: bfloat16 [128, 8192], P('chan', 'atoms'), may hold values from -6 to 6
- positions: float32 [3, 8192], P(None, 'atoms'), may hold values from 0 to 256
- block_counts: int32 [64], P('atoms'), may hold values from 64 to 128
- radial_w: float32 [8, 3, 128], P(None, None, 'chan'), may hold values from -2 to 2
- mix_w: bfloat16 [4, 128, 128], replicated, may hold values from -0.25 to 0.25
- read_w: float32 [128], P('chan'), may hold values from -0.5 to 0.5
- ghost_lists: int32 [16, 2, 2], P('atoms'), may hold values from 0 to 3, as said below
- tile_pairs: int32 [16, 24, 2], P('atoms'), may hold values from 0 to 7, as said below
- tile_count: int32 [16], P('atoms'), may hold values from 9 to 24, as said below
Outputs:
- updated: bfloat16 [128, 8192], P('chan', 'atoms')
- energies: float32 [8192], P('atoms')
- scale: float32 [], replicated
The draws below stay inside these ranges and needn't reach their ends.
Inputs may be any that keep to these rules, and one draw needn't show every extreme that they name: `ghost_lists`: row 0 of group g lists each of its even-numbered blocks once and row 1 each odd-numbered block once, in some order. `tile_pairs`: codes below 4 name the group's own block, codes 4 to 5 a slot of the previous group's ghost_lists row 1, higher codes a slot of the next group's row 0; no code points outside the first or last group. Tile t < 4 of each group is (t, t). Tiles from tile_count[g] on are (0, 0). `tile_count`: some group has 24 live tiles.
All inputs are finite; a program needn't handle non-finite values.
Results may differ from the reference program's by a relative error of at most 0.007.
Values may be sent and summed in bfloat16 or wider, within the bound.
A program may use at most 64 MiB of HBM per device.

```python
import math
import jax
import jax.numpy as jnp
from jax import lax

C = 128
NR = 8
BLK = 128
BLK_DEV = 4
GHOST = 2
TILES_DEV = 24
SHARDS = 16
BLOCKS = 64
ATOMS = 8192


pitch_across = 3.0


def draw_positions(key, part):
    atom = jnp.arange(ATOMS, dtype=jnp.int32)
    block = atom // BLK
    group = block // BLK_DEV
    local = block % BLK_DEV
    column = local // 2
    cells = jnp.stack([2 * group + local % 2, column // 2, column % 2]).astype(jnp.float32)
    jitter = jax.random.uniform(jax.random.fold_in(key, 3), (3, ATOMS), jnp.float32)
    pitch_side = math.sqrt(BLK * 4.0 / 3.0)
    pitches = jnp.array([pitch_across, pitch_side, pitch_side], jnp.float32)
    return (cells + jitter) * pitches[:, None]


def ghost_rows(key):
    subkeys = jax.random.split(jax.random.fold_in(key, 5), SHARDS * 2)
    orders = jax.vmap(lambda subkey: jax.random.permutation(subkey, GHOST))(subkeys).reshape(SHARDS, 2, GHOST)
    return (2 * orders + jnp.arange(2, dtype=jnp.int32)[None, :, None]).astype(jnp.int32)


def draw_ghost_lists(key, part):
    return ghost_rows(key)


def draw_tile_count(key, part):
    lowest = BLK_DEV + (TILES_DEV - BLK_DEV) // 4
    counts = jax.random.randint(jax.random.fold_in(key, 7), (SHARDS,), lowest, TILES_DEV + 1)
    fullest = jax.random.randint(jax.random.fold_in(key, 8), (), 0, SHARDS)
    return jnp.where(jnp.arange(SHARDS) == fullest, TILES_DEV, counts).astype(jnp.int32)


def draw_tile_pairs(key, part):
    counts = draw_tile_count(key, part)
    lists = ghost_rows(key)
    subkeys = jax.random.split(jax.random.fold_in(key, 9), SHARDS)
    slots = jnp.arange(GHOST, dtype=jnp.int32)

    def one_group(subkey, device, total):
        pieces = jax.random.split(subkey, 3)
        places = jnp.arange(TILES_DEV)
        receivers = jax.random.randint(pieces[0], (TILES_DEV,), 0, BLK_DEV)
        moves = jax.random.randint(pieces[1], (TILES_DEV, 3), -1, 2)
        forced = (places >= BLK_DEV) & (places < BLK_DEV + 4)
        side = (places - BLK_DEV) % 2
        forced_column = jax.random.randint(pieces[2], (TILES_DEV,), 0, GHOST)
        receivers = jnp.where(forced, 2 * forced_column + side, receivers)
        forced_moves = jnp.stack([2 * side - 1, jnp.zeros_like(side), jnp.zeros_like(side)], axis=-1)
        moves = jnp.where(forced[:, None], forced_moves, moves)
        column = receivers // 2
        cell_x = 2 * device + receivers % 2 + moves[:, 0]
        cell_y = column // 2 + moves[:, 1]
        cell_z = column % 2 + moves[:, 2]
        target_column = 2 * cell_y + cell_z
        valid = (cell_y >= 0) & (cell_z >= 0) & (cell_z <= 1) & (target_column < GHOST) & (cell_x >= 0) & (cell_x < 2 * SHARDS)
        target_group = jnp.where(valid, cell_x // 2, device)
        target_block = jnp.clip(2 * target_column + cell_x % 2, 0, BLK_DEV - 1)
        left_row = lists[jnp.maximum(device - 1, 0), 1]
        right_row = lists[jnp.minimum(device + 1, SHARDS - 1), 0]
        left_slot = jnp.sum(jnp.where(left_row[None, :] == target_block[:, None], slots[None, :], 0), axis=1)
        right_slot = jnp.sum(jnp.where(right_row[None, :] == target_block[:, None], slots[None, :], 0), axis=1)
        codes = jnp.where(target_group == device, target_block, jnp.where(target_group == device - 1, BLK_DEV + left_slot, BLK_DEV + GHOST + right_slot))
        codes = jnp.where(valid, codes, receivers)
        receivers = jnp.where(places < BLK_DEV, places, receivers)
        codes = jnp.where(places < BLK_DEV, places, codes)
        living = places < total
        receivers = jnp.where(living, receivers, 0)
        codes = jnp.where(living, codes, 0)
        return jnp.stack([receivers, codes], axis=-1)
    return jax.vmap(one_group)(subkeys, jnp.arange(SHARDS), counts).astype(jnp.int32)


def with_ends(drawn, rng, smallest, high):
    longest = drawn.shape.index(max(drawn.shape))
    spots = []
    for shift in (0, 1):
        where = [jax.random.randint(jax.random.fold_in(rng, axis), (), 0, length) for axis, length in enumerate(drawn.shape)]
        where[longest] = (where[longest] + shift) % drawn.shape[longest]
        spots.append(tuple(where))
    return drawn.at[spots[0]].set(smallest).at[spots[1]].set(high)


def block_scale(rng, dims, cuts, smallest, largest):
    factor_of, own = 1.0, jax.random.fold_in(rng, 6)
    for dim, blocks in cuts:
        draws = jnp.exp(jax.random.uniform(jax.random.fold_in(own, dim), (blocks,), jnp.float32, smallest / len(cuts), largest / len(cuts)))
        factor_of = factor_of * jnp.repeat(draws, dims[dim] // blocks).reshape([-1 if axis == dim else 1 for axis in range(len(dims))])
    return factor_of


def scatter_about(own_key, extent, spread, bound, shards=(), kind=jnp.bfloat16):
    entries = spread * jax.random.normal(own_key, extent, jnp.float32)
    if shards:
        entries = entries * block_scale(own_key, extent, shards, -0.22, 0.18)
    return jnp.clip(entries, -bound, bound).astype(kind)


def setup_inputs(seed: int = 0) -> dict:
    keys = jax.random.split(jax.random.key(seed), 10)
    return {
        "features": scatter_about(keys[0], (C, ATOMS), 1.0, 6.0, ((0, 2), (1, 16))),
        "positions": draw_positions(jax.random.fold_in(keys[9], 71), 0),
        "block_counts": with_ends(jax.random.randint(keys[2], (BLOCKS,), BLK // 2, BLK + 1), jax.random.fold_in(keys[2], 1), BLK // 2, BLK).astype(jnp.int32),
        "radial_w": scatter_about(keys[3], (NR, 3, C), NR ** -0.5, 2.0, ((2, 2),), jnp.float32),
        "mix_w": scatter_about(keys[4], (4, C, C), (4 * C) ** -0.5, 0.25),
        "read_w": scatter_about(keys[5], (C,), C ** -0.5, 0.5, ((0, 2),), jnp.float32),
        "ghost_lists": draw_ghost_lists(jax.random.fold_in(keys[9], 71), 0),
        "tile_pairs": draw_tile_pairs(jax.random.fold_in(keys[9], 71), 0),
        "tile_count": draw_tile_count(jax.random.fold_in(keys[9], 71), 0),
    }


root_three = 3.0 ** 0.5
root_fifteen = 15.0 ** 0.5
half_root_five = 0.5 * 5.0 ** 0.5
half_root_fifteen = 0.5 * 15.0 ** 0.5
cutoff_square = 9.0
soften = 0.25
center_step = 3.0 / 7.0
radial_sharp = 2.0

def harmonics(unit_x, unit_y, unit_z):
    return jnp.stack([jnp.ones_like(unit_x), root_three * unit_x, root_three * unit_y, root_three * unit_z, root_fifteen * unit_x * unit_y, root_fifteen * unit_y * unit_z, half_root_five * (2.0 * unit_z * unit_z - unit_x * unit_x - unit_y * unit_y), root_fifteen * unit_x * unit_z, half_root_fifteen * (unit_x * unit_x - unit_y * unit_y)])

def tile_kernel(pos_recv, pos_send, self_pair):
    offset = pos_send[:, None, :] - pos_recv[:, :, None]
    dist_sq = lax.optimization_barrier(jnp.sum(offset * offset, axis=0))
    block_width = dist_sq.shape[0]
    diagonal = (lax.broadcasted_iota(jnp.int32, (block_width, block_width), 0) == lax.broadcasted_iota(jnp.int32, (block_width, block_width), 1)).astype(jnp.float32)
    cutoff = jnp.square(jnp.maximum(1.0 - dist_sq / cutoff_square, 0.0)) * (1.0 - self_pair * diagonal)
    distance = jnp.sqrt(dist_sq + soften)
    unit = offset / distance
    angular = harmonics(unit[0], unit[1], unit[2]) * cutoff
    centers = jnp.arange(NR, dtype=jnp.float32) * center_step
    radial = jnp.exp(-radial_sharp * jnp.square(distance[None] - centers[:, None, None]))
    return (radial[:, None] * angular[None]).astype(jnp.bfloat16)

def invariants(density):
    first = density[:, 0]
    return jnp.stack([first, first * first, lax.optimization_barrier(jnp.sum(jnp.square(density[:, 1:4]), axis=1)), lax.optimization_barrier(jnp.sum(jnp.square(density[:, 4:9]), axis=1))])

def reference(features, positions, block_counts, radial_w, mix_w, read_w, ghost_lists, tile_pairs, tile_count):
    present = (jnp.arange(BLK, dtype=jnp.int32)[None, :] < block_counts[:, None]).astype(jnp.float32)
    present_flat = present.reshape(-1)
    senders = (features.astype(jnp.float32) * present_flat[None, :]).astype(jnp.bfloat16)
    send_blocks = senders.reshape(C, BLOCKS, BLK)
    where_blocks = positions.astype(jnp.float32).reshape(3, BLOCKS, BLK)
    degree = jnp.array([0, 1, 1, 1, 2, 2, 2, 2, 2], dtype=jnp.int32)
    table = jnp.take(radial_w, degree, axis=1)
    tile_list = tile_pairs.reshape(SHARDS * TILES_DEV, 2)
    serial = jnp.arange(SHARDS * TILES_DEV, dtype=jnp.int32)
    owners = serial // TILES_DEV
    alive = (serial % TILES_DEV < tile_count[owners]).astype(jnp.float32)
    receivers = (owners * BLK_DEV + tile_list[:, 0]).astype(jnp.int32)
    codes = tile_list[:, 1]
    left_dev = jnp.maximum(owners - 1, 0)
    right_dev = jnp.minimum(owners + 1, SHARDS - 1)
    slot_left = jnp.clip(codes - BLK_DEV, 0, GHOST - 1)
    slot_right = jnp.clip(codes - BLK_DEV - GHOST, 0, GHOST - 1)
    from_left = left_dev * BLK_DEV + ghost_lists[left_dev, 1, slot_left]
    from_right = right_dev * BLK_DEV + ghost_lists[right_dev, 0, slot_right]
    sources = jnp.where(codes < BLK_DEV, owners * BLK_DEV + codes, jnp.where(codes < BLK_DEV + GHOST, from_left, from_right)).astype(jnp.int32)
    self_pairs = ((codes < BLK_DEV) & (codes == tile_list[:, 0])).astype(jnp.float32)

    def update(totals, item):
        receiver, source, self_pair, weight = item
        pos_recv = lax.dynamic_index_in_dim(where_blocks, receiver, 1, keepdims=False)
        pos_send = lax.dynamic_index_in_dim(where_blocks, source, 1, keepdims=False)
        sender_rows = lax.dynamic_index_in_dim(send_blocks, source, 1, keepdims=False)
        kernel = tile_kernel(pos_recv, pos_send, self_pair)
        partial_sums = jnp.einsum('cj,kmij->ckmi', sender_rows.astype(jnp.float32), kernel.astype(jnp.float32))
        term = jnp.einsum('kmc,ckmi->cmi', table, partial_sums, precision=lax.Precision.HIGHEST)
        return (totals.at[receiver].add(term * weight), None)
    start = jnp.zeros((BLOCKS, C, 9, BLK), jnp.float32)
    totals = lax.scan(update, start, (receivers, sources, self_pairs, alive))[0]
    density = totals.transpose(1, 2, 0, 3).reshape(C, 9, ATOMS)
    basis = invariants(density).astype(jnp.bfloat16)
    mixed = jnp.einsum('qco,qca->oa', mix_w.astype(jnp.float32), basis.astype(jnp.float32))
    hidden = features.astype(jnp.float32) + jax.nn.silu(mixed)
    updated = (hidden * present_flat[None, :]).astype(jnp.bfloat16)
    energy = jnp.dot(read_w, hidden, precision=lax.Precision.HIGHEST)
    total_square = jnp.sum(present_flat * energy * energy)
    total_atoms = jnp.sum(present_flat)
    scale = jnp.sqrt(1.0 + total_square / total_atoms)
    return (updated, energy * present_flat / scale, scale)
```

```python
import functools

import jax
import jax.numpy as jnp
from jax import lax
from jax.experimental import pallas as pl
from jax.experimental.pallas import tpu as pltpu
from jax.sharding import PartitionSpec as P

root_three = 3.0**0.5
root_fifteen = 15.0**0.5
half_root_five = 0.5 * 5.0**0.5
half_root_fifteen = 0.5 * 15.0**0.5
cutoff_square = 9.0
soften = 0.25
center_step = 3.0 / 7.0
radial_sharp = 2.0
degrees = ((0,), (1, 2, 3), (4, 5, 6, 7, 8))
MESH = pl.DeviceIdType.MESH


def gather_kernel(
    shape, blocks, feat_ref, place_ref, w_ref, feats, places, walls, sems_s, sems_r, local_sems
):
    groups, peers = shape
    g, h = lax.axis_index("atoms"), lax.axis_index("chan")
    chans, width = feat_ref.shape[0], feat_ref.shape[1] // blocks
    after, before = lax.rem(g + 1, groups), lax.rem(g + groups - 1, groups)
    barrier = pltpu.get_barrier_semaphore()
    for d in range(1, peers):
        pl.semaphore_signal(
            barrier, inc=1, device_id=(g, lax.rem(h + d, peers)), device_id_type=MESH
        )
    for there in (after, before):
        for d in range(peers):
            pl.semaphore_signal(
                barrier, inc=1, device_id=(there, lax.rem(h + d, peers)), device_id_type=MESH
            )
    rows = pl.ds(pl.multiple_of(h * chans, chans), chans)
    own = pl.ds(0, blocks * width)
    locals_ = [
        pltpu.make_async_copy(feat_ref, feats.at[rows, own], local_sems.at[0]),
        pltpu.make_async_copy(w_ref, walls.at[h], local_sems.at[1]),
    ]
    for copy in locals_:
        copy.start()
    pl.semaphore_wait(barrier, 3 * peers - 1)
    copies = []

    def send(src, dst, device):
        slot = len(copies)
        copy = pltpu.make_async_remote_copy(
            src_ref=src,
            dst_ref=dst,
            send_sem=sems_s.at[slot],
            recv_sem=sems_r.at[slot],
            device_id=device,
            device_id_type=MESH,
        )
        copy.start()
        copies.append(copy)

    half = blocks // 2
    for d in range(peers):
        to = lax.rem(h + d, peers)
        for n in range(half):
            for there, block, slot in (
                (after, 2 * n + 1, blocks + n),
                (before, 2 * n, blocks + half + n),
            ):
                send(
                    feat_ref.at[:, pl.ds(block * width, width)],
                    feats.at[rows, pl.ds(slot * width, width)],
                    (there, to),
                )
    send(place_ref, places.at[0], (after, h))
    send(place_ref, places.at[1], (before, h))
    for d in range(1, peers):
        to = (g, lax.rem(h + d, peers))
        send(feat_ref, feats.at[rows, own], to)
        send(w_ref, walls.at[h], to)
    for copy in locals_:
        copy.wait()
    for copy in copies:
        copy.wait()


def compute_kernel(
    peers, blocks, basis_count, pairs, count, feats, place, places, walls, mix, upd, stats,
    table, spos, rpos, feat_rows, acc,
):
    h = lax.axis_index("chan")
    width = feats.shape[1] // (2 * blocks)
    part = width // peers
    half = blocks // 2
    mine = pl.ds(pl.multiple_of(h * part, part), part)
    w = jnp.concatenate([walls[n] for n in range(peers)], axis=1)
    atom = lax.broadcasted_iota(jnp.int32, (width, 1), 0).astype(jnp.float32)

    def block_of(slot):
        return feats[:, slot * width : (slot + 1) * width].astype(jnp.float32)

    def store_source(code, rows, present):
        masked = jnp.where(atom < present, rows, 0.0)
        for l in range(3):
            for k in range(basis_count):
                table[code, l, k * width : (k + 1) * width, :] = (
                    masked * w[3 * k + l : 3 * k + l + 1, :]
                ).astype(jnp.bfloat16)

    for b in range(blocks):
        rows = block_of(b).T
        feat_rows[b] = rows
        store_source(b, rows, place[3:4, b : b + 1])
        spos[b] = place[:, b * width : (b + 1) * width]
        for axis in range(3):
            rpos[3 * b + axis] = jnp.broadcast_to(
                place[axis : axis + 1, b * width : (b + 1) * width], (width, width)
            ).T
    for side in range(2):
        near = places.at[side]
        for n in range(half):
            column = blocks + (1 - side) * half + n
            listed = near[3:4, column : column + 1]
            code = blocks + side * half + n
            rows, where, present = None, None, None
            for m in range(half):
                block = 2 * m + 1 - side
                is_it = listed == float(block)
                new = (
                    block_of(blocks + side * half + m),
                    near[:, block * width : (block + 1) * width],
                    near[3:4, block : block + 1],
                )
                if m == 0:
                    rows, where, present = new
                else:
                    rows = jnp.where(is_it, new[0], rows)
                    where = jnp.where(is_it, new[1], where)
                    present = jnp.where(is_it, new[2], present)
            store_source(code, rows.T, present)
            spos[code] = where
    acc[...] = jnp.zeros_like(acc)
    diagonal = (
        lax.broadcasted_iota(jnp.int32, (part, width), 0) + h * part
        == lax.broadcasted_iota(jnp.int32, (part, width), 1)
    ).astype(jnp.float32)

    def one_tile(t, carry):
        r, q = pairs[0, t, 0], pairs[0, t, 1]
        dx = spos[q, 0:1, :] - rpos[3 * r, mine, :]
        dy = spos[q, 1:2, :] - rpos[3 * r + 1, mine, :]
        dz = spos[q, 2:3, :] - rpos[3 * r + 2, mine, :]
        d2 = dx * dx + dy * dy + dz * dz
        is_self = (r == q).astype(jnp.float32)
        edge = jnp.maximum(1.0 - d2 * (1.0 / cutoff_square), 0.0)
        cut = edge * edge * (1.0 - is_self * diagonal)
        inverse = lax.rsqrt(d2 + soften)
        dist = (d2 + soften) * inverse
        x, y, z = dx * inverse, dy * inverse, dz * inverse
        cx, cy = cut * root_fifteen * x, cut * root_fifteen * y
        cut3 = cut * root_three
        angular = (
            cut,
            cut3 * x,
            cut3 * y,
            cut3 * z,
            cx * y,
            cy * z,
            cut * half_root_five * (2.0 * z * z - x * x - y * y),
            cx * z,
            cut * half_root_fifteen * (x * x - y * y),
        )
        radial = []
        for k in range(basis_count):
            off = dist - center_step * k
            radial.append(jnp.exp(-radial_sharp * off * off))
        for l, ms in enumerate(degrees):
            lhs = jnp.concatenate(
                [
                    jnp.concatenate(
                        [(radial[k] * angular[m]).astype(jnp.bfloat16) for k in range(basis_count)],
                        axis=1,
                    )
                    for m in ms
                ],
                axis=0,
            )
            span = slice(ms[0] * part, (ms[-1] + 1) * part)
            acc[r, span, :] += jnp.dot(
                lhs, table[q, l], preferred_element_type=jnp.float32
            )
        return carry

    lax.fori_loop(0, count[0], one_tile, 0)
    basis = [[], [], [], []]
    for b in range(blocks):
        d = [acc[b, m * part : (m + 1) * part, :] for m in range(9)]
        values = (
            d[0],
            d[0] * d[0],
            d[1] * d[1] + d[2] * d[2] + d[3] * d[3],
            d[4] * d[4] + d[5] * d[5] + d[6] * d[6] + d[7] * d[7] + d[8] * d[8],
        )
        for kept, value in zip(basis, values):
            kept.append(value.astype(jnp.bfloat16))
    mixed = None
    for q in range(4):
        term = jnp.dot(
            jnp.concatenate(basis[q], axis=0), mix[q], preferred_element_type=jnp.float32
        )
        mixed = term if mixed is None else mixed + term
    mixed = mixed / (1.0 + jnp.exp(-mixed))
    feat = jnp.concatenate([feat_rows[b, mine, :] for b in range(blocks)], axis=0)
    hidden = feat + mixed
    my_atom = (lax.broadcasted_iota(jnp.int32, (part, 1), 0) + h * part).astype(jnp.float32)
    present = jnp.concatenate(
        [(my_atom < place[3:4, b : b + 1]).astype(jnp.float32) for b in range(blocks)], axis=0
    )
    hidden = hidden * present
    upd[...] = hidden.T.astype(jnp.bfloat16)
    energy = jnp.sum((hidden * w[3 * basis_count : 3 * basis_count + 1, :]).T, axis=0, keepdims=True)
    square = jnp.sum(energy * energy, axis=1, keepdims=True)
    atoms = jnp.sum(present, axis=0, keepdims=True)
    stats[...] = jnp.zeros_like(stats)
    stats[0:1, :] = energy
    stats[1:2, :] = jnp.broadcast_to(square, energy.shape)
    stats[2:3, :] = jnp.broadcast_to(atoms, energy.shape)


def return_kernel(
    shape, blocks, upd, stats, updated, energies, scale_ref,
    rows_in, stats_in, group_sum, sums_in, sems_s, sems_r, sums_s, sums_r,
):
    groups, peers = shape
    g, h = lax.axis_index("atoms"), lax.axis_index("chan")
    chans = updated.shape[0]
    part = upd.shape[1] // blocks
    barrier = pltpu.get_barrier_semaphore()
    for d in range(1, peers):
        pl.semaphore_signal(
            barrier, inc=1, device_id=(g, lax.rem(h + d, peers)), device_id_type=MESH
        )

    def greet(d, carry):
        pl.semaphore_signal(
            barrier, inc=1, device_id=(lax.rem(g + d, groups), h), device_id_type=MESH
        )
        return carry

    lax.fori_loop(1, groups, greet, 0)
    pl.semaphore_wait(barrier, peers + groups - 2)
    copies = []

    def send(src, dst, device):
        slot = len(copies)
        copy = pltpu.make_async_remote_copy(
            src_ref=src,
            dst_ref=dst,
            send_sem=sems_s.at[slot],
            recv_sem=sems_r.at[slot],
            device_id=device,
            device_id_type=MESH,
        )
        copy.start()
        copies.append(copy)

    for d in range(1, peers):
        send(stats, stats_in.at[h], (g, lax.rem(h + d, peers)))
    for d in range(1, peers):
        to = lax.rem(h + d, peers)
        send(
            upd.at[pl.ds(pl.multiple_of(to * chans, chans), chans), :],
            rows_in.at[h],
            (g, to),
        )
    stats_in[h] = stats[...]
    rows_in[h] = upd[pl.ds(pl.multiple_of(h * chans, chans), chans), :]
    for copy in copies[: peers - 1]:
        copy.wait()
    total = stats_in[0]
    for n in range(1, peers):
        total = total + stats_in[n]
    group_sum[...] = jnp.broadcast_to(total[:, 0:1], group_sum.shape)

    def sum_copy(d):
        return pltpu.make_async_remote_copy(
            src_ref=group_sum,
            dst_ref=sums_in.at[d],
            send_sem=sums_s.at[d],
            recv_sem=sums_r.at[d],
            device_id=(lax.rem(g + d, groups), h),
            device_id_type=MESH,
        )

    def start(d, carry):
        sum_copy(d).start()
        return carry

    lax.fori_loop(1, groups, start, 0)
    for copy in copies[peers - 1 :]:
        copy.wait()
    pieces = [rows_in[n].astype(jnp.float32) for n in range(peers)]
    for b in range(blocks):
        span = slice(b * part, (b + 1) * part)
        updated[:, b * part * peers : (b + 1) * part * peers] = jnp.concatenate(
            [piece[:, span] for piece in pieces], axis=1
        ).astype(jnp.bfloat16)
    energy = jnp.concatenate(
        [
            stats_in[n][:, b * part : (b + 1) * part]
            for b in range(blocks)
            for n in range(peers)
        ],
        axis=1,
    )[0:1, :]

    def finish(d, whole):
        sum_copy(d).wait()
        return whole + sums_in[d]

    whole = lax.fori_loop(1, groups, finish, group_sum[...])
    scale = jnp.sqrt(1.0 + whole[1:2, :] / whole[2:3, :])
    energies[...] = energy / scale[:, 0:1]
    scale_ref[...] = scale


def per_device(
    shape, features, positions, block_counts, radial_w, mix_w, read_w, ghost_lists, tile_pairs,
    tile_count,
):
    groups, peers = shape
    chans, atoms = features.shape
    blocks = block_counts.shape[0]
    width = atoms // blocks
    basis_count = radial_w.shape[0]
    channels = mix_w.shape[1]
    part = width // peers
    f32 = jnp.float32
    extra = jnp.concatenate([block_counts, ghost_lists.reshape(-1)]).astype(f32)
    place = jnp.concatenate(
        [positions, jnp.pad(extra, (0, atoms - extra.shape[0]))[None], jnp.zeros((4, atoms), f32)]
    )
    weights = jnp.concatenate(
        [radial_w.reshape(-1, chans), read_w[None], jnp.zeros((7, chans), f32)]
    )
    vmem = pl.BlockSpec(memory_space=pltpu.VMEM)
    smem = pl.BlockSpec(memory_space=pltpu.SMEM)
    dma = pltpu.SemaphoreType.DMA
    first = 2 * peers * (blocks // 2) + 2 + 2 * (peers - 1)
    feats, places, walls = pl.pallas_call(
        functools.partial(gather_kernel, shape, blocks),
        out_shape=(
            jax.ShapeDtypeStruct((channels, 2 * atoms), jnp.bfloat16),
            jax.ShapeDtypeStruct((2,) + place.shape, f32),
            jax.ShapeDtypeStruct((peers,) + weights.shape, f32),
        ),
        in_specs=[vmem] * 3,
        out_specs=(vmem,) * 3,
        scratch_shapes=[dma((first,)), dma((first,)), dma((2,))],
        compiler_params=pltpu.CompilerParams(collective_id=0, has_side_effects=True),
        name="gather",
    )(features, place, weights)
    upd, stats = pl.pallas_call(
        functools.partial(compute_kernel, peers, blocks, basis_count),
        out_shape=(
            jax.ShapeDtypeStruct((channels, blocks * part), jnp.bfloat16),
            jax.ShapeDtypeStruct((8, blocks * part), f32),
        ),
        in_specs=[smem, smem] + [vmem] * 5,
        out_specs=(vmem, vmem),
        scratch_shapes=[
            pltpu.VMEM((2 * blocks, 3, basis_count * width, channels), jnp.bfloat16),
            pltpu.VMEM((2 * blocks, 8, width), f32),
            pltpu.VMEM((3 * blocks, width, width), f32),
            pltpu.VMEM((blocks, width, channels), f32),
            pltpu.VMEM((blocks, 9 * part, channels), f32),
        ],
        compiler_params=pltpu.CompilerParams(vmem_limit_bytes=50 * 1024 * 1024),
        name="compute",
    )(tile_pairs, tile_count, feats, place, places, walls, mix_w)
    last = 2 * (peers - 1)
    updated, energies, scale = pl.pallas_call(
        functools.partial(return_kernel, shape, blocks),
        out_shape=(
            jax.ShapeDtypeStruct((chans, atoms), jnp.bfloat16),
            jax.ShapeDtypeStruct((1, atoms), f32),
            jax.ShapeDtypeStruct((1, 128), f32),
        ),
        in_specs=[vmem] * 2,
        out_specs=(vmem,) * 3,
        scratch_shapes=[
            pltpu.VMEM((peers, chans, blocks * part), jnp.bfloat16),
            pltpu.VMEM((peers, 8, blocks * part), f32),
            pltpu.VMEM((8, 128), f32),
            pltpu.VMEM((groups, 8, 128), f32),
            dma((last,)),
            dma((last,)),
            dma((groups,)),
            dma((groups,)),
        ],
        compiler_params=pltpu.CompilerParams(collective_id=1, has_side_effects=True),
        name="hand_back",
    )(upd, stats)
    return updated, energies.reshape(-1), scale[0, 0]


def solution(mesh):
    shape = (mesh.shape["atoms"], mesh.shape["chan"])
    in_specs = (
        P("chan", "atoms"),
        P(None, "atoms"),
        P("atoms"),
        P(None, None, "chan"),
        P(),
        P("chan"),
        P("atoms", None, None),
        P("atoms", None, None),
        P("atoms"),
    )
    out_specs = (P("chan", "atoms"), P("atoms"), P())
    return jax.shard_map(
        functools.partial(per_device, shape),
        mesh=mesh,
        in_specs=in_specs,
        out_specs=out_specs,
        check_vma=False,
    )
```

```python
import functools

import jax
import jax.numpy as jnp
from jax import lax
from jax.experimental import pallas as pl
from jax.experimental.pallas import tpu as pltpu
from jax.sharding import PartitionSpec as P

root_three = 3.0**0.5
root_fifteen = 15.0**0.5
half_root_five = 0.5 * 5.0**0.5
half_root_fifteen = 0.5 * 15.0**0.5
cutoff_square = 9.0
soften = 0.25
center_step = 3.0 / 7.0
radial_sharp = 2.0
degrees = ((0,), (1, 2, 3), (4, 5, 6, 7, 8))
MESH = pl.DeviceIdType.MESH


def layer_kernel(
    shape, basis_count, pairs, count, feat_ref, where_ref, present_ref, list_ref, radial_ref,
    read_ref, mix, updated, energies, scale_ref,
    own_in, ghost_in, where_in, present_in, list_in, radial_in, read_in,
    table, spos, rpos, feat_rows, terms, upd, stats, rows_in, stats_in, group_sum, sums_in,
    local_sems, near_s, near_r, far_s, far_r, last_s, last_r, sums_s, sums_r,
):
    groups, peers = shape
    g, h = lax.axis_index("atoms"), lax.axis_index("chan")
    chans = feat_ref.shape[0]
    blocks = present_ref.shape[1]
    half = list_ref.shape[1]
    width = feat_ref.shape[1] // blocks
    tiles = pairs.shape[1]
    part = width // peers
    after, before = lax.rem(g + 1, groups), lax.rem(g + groups - 1, groups)
    barrier = pltpu.get_barrier_semaphore()

    def signal(device):
        pl.semaphore_signal(barrier, inc=1, device_id=device, device_id_type=MESH)

    for d in range(1, peers):
        to = lax.rem(h + d, peers)
        signal((g, to))
        signal((after, to))
        signal((before, to))

    def greet(d, carry):
        signal((lax.rem(g + d, groups), h))
        return carry

    lax.fori_loop(1, groups, greet, 0)
    locals_ = [
        pltpu.make_async_copy(feat_ref, own_in.at[h], local_sems.at[0]),
        pltpu.make_async_copy(radial_ref, radial_in.at[h], local_sems.at[1]),
        pltpu.make_async_copy(read_ref, read_in.at[h], local_sems.at[2]),
    ]
    for copy in locals_:
        copy.start()
    pl.semaphore_wait(barrier, 3 * (peers - 1) + groups - 1)

    def send(copies, sems, src, dst, device):
        slot = len(copies)
        copy = pltpu.make_async_remote_copy(
            src_ref=src,
            dst_ref=dst,
            send_sem=sems[0].at[slot],
            recv_sem=sems[1].at[slot],
            device_id=device,
            device_id_type=MESH,
        )
        copy.start()
        copies.append(copy)

    near, far, last = [], [], []
    for d in range(1, peers):
        to = (g, lax.rem(h + d, peers))
        send(near, (near_s, near_r), feat_ref, own_in.at[h], to)
        send(near, (near_s, near_r), radial_ref, radial_in.at[h], to)
        send(near, (near_s, near_r), read_ref, read_in.at[h], to)
    for d in range(peers):
        to = lax.rem(h + d, peers)
        for n in range(half):
            for side, there in ((0, after), (1, before)):
                block = 2 * n + 1 - side
                send(
                    far,
                    (far_s, far_r),
                    feat_ref.at[:, pl.ds(block * width, width)],
                    ghost_in.at[side * half + n, h],
                    (there, to),
                )
    for side, there in ((0, after), (1, before)):
        send(far, (far_s, far_r), where_ref, where_in.at[side], (there, h))
        send(far, (far_s, far_r), present_ref, present_in.at[side], (there, h))
        send(far, (far_s, far_r), list_ref, list_in.at[side], (there, h))

    mine = pl.ds(pl.multiple_of(h * part, part), part)
    atom = lax.broadcasted_iota(jnp.int32, (width, 1), 0)
    for b in range(blocks):
        spos[b, 0:3, :] = where_ref[:, b * width : (b + 1) * width]
        for axis in range(3):
            rpos[3 * b + axis] = jnp.broadcast_to(
                where_ref[axis : axis + 1, b * width : (b + 1) * width], (width, width)
            ).T
    diagonal = (
        lax.broadcasted_iota(jnp.int32, (part, width), 0) + h * part
        == lax.broadcasted_iota(jnp.int32, (part, width), 1)
    ).astype(jnp.float32)
    terms[0] = jnp.zeros_like(terms[0])
    for copy in locals_:
        copy.wait()
    for copy in near:
        copy.wait()
    weights = [
        jnp.concatenate([radial_in[n, l] for n in range(peers)], axis=1) for l in range(3)
    ]
    read = jnp.concatenate([read_in[n] for n in range(peers)], axis=1)

    def store_source(code, rows, present):
        masked = jnp.where(atom < present, rows, 0.0)
        for l in range(3):
            for k in range(basis_count):
                table[code, l, k * width : (k + 1) * width, :] = (
                    masked * weights[l][k : k + 1, :]
                ).astype(jnp.bfloat16)

    for b in range(blocks):
        rows = jnp.concatenate(
            [own_in[n, :, b * width : (b + 1) * width] for n in range(peers)], axis=0
        ).astype(jnp.float32).T
        feat_rows[b] = rows
        store_source(b, rows, present_ref[0:1, b : b + 1])

    def one_tile(t, lasts):
        r, q = pairs[0, t], pairs[1, t]
        dx = spos[q, 0:1, :] - rpos[3 * r, mine, :]
        dy = spos[q, 1:2, :] - rpos[3 * r + 1, mine, :]
        dz = spos[q, 2:3, :] - rpos[3 * r + 2, mine, :]
        d2 = dx * dx + dy * dy + dz * dz
        is_self = (r == q).astype(jnp.float32)
        alive = (t < count[0]).astype(jnp.float32)
        edge = jnp.maximum(1.0 - d2 * (1.0 / cutoff_square), 0.0)
        cut = edge * edge * (alive - alive * is_self * diagonal)
        inverse = lax.rsqrt(d2 + soften)
        dist = (d2 + soften) * inverse
        x, y, z = dx * inverse, dy * inverse, dz * inverse
        cx, cy = cut * root_fifteen * x, cut * root_fifteen * y
        cut3 = cut * root_three
        angular = (
            cut,
            cut3 * x,
            cut3 * y,
            cut3 * z,
            cx * y,
            cy * z,
            cut * half_root_five * (2.0 * z * z - x * x - y * y),
            cx * z,
            cut * half_root_fifteen * (x * x - y * y),
        )
        radial = []
        for k in range(basis_count):
            off = dist - center_step * k
            radial.append(jnp.exp(-radial_sharp * off * off))
        previous = lasts[0]
        for b in range(1, blocks):
            previous = jnp.where(r == b, lasts[b], previous)
        for l, ms in enumerate(degrees):
            lhs = jnp.concatenate(
                [
                    jnp.concatenate(
                        [(radial[k] * angular[m]).astype(jnp.bfloat16) for k in range(basis_count)],
                        axis=1,
                    )
                    for m in ms
                ],
                axis=0,
            )
            span = slice(ms[0] * part, (ms[-1] + 1) * part)
            terms[t + 1, span, :] = terms[previous, span, :] + jnp.dot(
                lhs, table[q, l], preferred_element_type=jnp.float32
            )
        return tuple(jnp.where(r == b, t + 1, kept) for b, kept in enumerate(lasts))

    lasts = lax.fori_loop(0, blocks, one_tile, (jnp.int32(0),) * blocks)
    for copy in far:
        copy.wait()
    for side in range(2):
        for n in range(half):
            listed = list_in[side, 1 - side : 2 - side, n : n + 1]
            code = blocks + side * half + n
            rows, where, present = None, None, None
            for m in range(half):
                block = 2 * m + 1 - side
                new = (
                    jnp.concatenate(
                        [ghost_in[side * half + m, p] for p in range(peers)], axis=0
                    ).astype(jnp.float32),
                    where_in[side, :, block * width : (block + 1) * width],
                    present_in[side, 0:1, block : block + 1],
                )
                if m == 0:
                    rows, where, present = new
                else:
                    is_it = listed == block
                    rows = jnp.where(is_it, new[0], rows)
                    where = jnp.where(is_it, new[1], where)
                    present = jnp.where(is_it, new[2], present)
            store_source(code, rows.T, present)
            spos[code, 0:3, :] = where
    lasts = lax.fori_loop(blocks, tiles, one_tile, lasts)

    basis = [[], [], [], []]
    for b in range(blocks):
        d = [terms[lasts[b], m * part : (m + 1) * part, :] for m in range(9)]
        values = (
            d[0],
            d[0] * d[0],
            d[1] * d[1] + d[2] * d[2] + d[3] * d[3],
            d[4] * d[4] + d[5] * d[5] + d[6] * d[6] + d[7] * d[7] + d[8] * d[8],
        )
        for kept, value in zip(basis, values):
            kept.append(value.astype(jnp.bfloat16))
    mixed = None
    for q in range(4):
        term = jnp.dot(
            jnp.concatenate(basis[q], axis=0), mix[q], preferred_element_type=jnp.float32
        )
        mixed = term if mixed is None else mixed + term
    mixed = mixed / (1.0 + jnp.exp(-mixed))
    feat = jnp.concatenate([feat_rows[b, mine, :] for b in range(blocks)], axis=0)
    my_atom = lax.broadcasted_iota(jnp.int32, (part, 1), 0) + h * part
    present = jnp.concatenate(
        [(my_atom < present_ref[0:1, b : b + 1]).astype(jnp.float32) for b in range(blocks)],
        axis=0,
    )
    hidden = (feat + mixed) * present
    energy = jnp.sum((hidden * read).T, axis=0, keepdims=True)
    square = jnp.sum(energy * energy, axis=1, keepdims=True)
    atoms = jnp.sum(present, axis=0, keepdims=True)
    stats[...] = jnp.concatenate(
        [
            energy,
            jnp.broadcast_to(square, energy.shape),
            jnp.broadcast_to(atoms, energy.shape),
            jnp.zeros((5, energy.shape[1]), jnp.float32),
        ],
        axis=0,
    )
    upd[...] = hidden.T.astype(jnp.bfloat16)
    for d in range(1, peers):
        send(last, (last_s, last_r), stats, stats_in.at[h], (g, lax.rem(h + d, peers)))
    for d in range(1, peers):
        to = lax.rem(h + d, peers)
        send(
            last,
            (last_s, last_r),
            upd.at[pl.ds(pl.multiple_of(to * chans, chans), chans), :],
            rows_in.at[h],
            (g, to),
        )
    stats_in[h] = stats[...]
    rows_in[h] = upd[pl.ds(pl.multiple_of(h * chans, chans), chans), :]
    for copy in last[: peers - 1]:
        copy.wait()
    total = stats_in[0]
    for n in range(1, peers):
        total = total + stats_in[n]
    group_sum[...] = jnp.broadcast_to(total[:, 0:1], group_sum.shape)

    def sum_copy(d):
        return pltpu.make_async_remote_copy(
            src_ref=group_sum,
            dst_ref=sums_in.at[g],
            send_sem=sums_s.at[d],
            recv_sem=sums_r.at[d],
            device_id=(lax.rem(g + d, groups), h),
            device_id_type=MESH,
        )

    def start(d, carry):
        sum_copy(d).start()
        return carry

    lax.fori_loop(1, groups, start, 0)
    sums_in[g] = group_sum[...]
    for copy in last[peers - 1 :]:
        copy.wait()
    pieces = [rows_in[n].astype(jnp.float32) for n in range(peers)]
    for b in range(blocks):
        span = slice(b * part, (b + 1) * part)
        updated[:, b * part * peers : (b + 1) * part * peers] = jnp.concatenate(
            [piece[:, span] for piece in pieces], axis=1
        ).astype(jnp.bfloat16)
    energy = jnp.concatenate(
        [
            stats_in[n][:, b * part : (b + 1) * part]
            for b in range(blocks)
            for n in range(peers)
        ],
        axis=1,
    )[0:1, :]

    def finish(d, carry):
        sum_copy(d).wait()
        return carry

    lax.fori_loop(1, groups, finish, 0)
    whole = jnp.sum(sums_in[...], axis=0)
    scale = jnp.sqrt(1.0 + whole[1:2, :] / whole[2:3, :])
    energies[...] = energy / scale[:, 0:1]
    scale_ref[...] = scale


def per_device(
    shape, features, positions, block_counts, radial_w, mix_w, read_w, ghost_lists, tile_pairs,
    tile_count,
):
    groups, peers = shape
    chans, atoms = features.shape
    blocks = block_counts.shape[0]
    half = ghost_lists.shape[2]
    width = atoms // blocks
    basis_count = radial_w.shape[0]
    channels = mix_w.shape[1]
    tiles = tile_pairs.shape[1]
    part = width // peers
    f32, bf16, i32 = jnp.float32, jnp.bfloat16, jnp.int32
    vmem = pl.BlockSpec(memory_space=pltpu.VMEM)
    smem = pl.BlockSpec(memory_space=pltpu.SMEM)
    dma = pltpu.SemaphoreType.DMA
    near, far, last = 3 * (peers - 1), 2 * peers * half + 6, 2 * (peers - 1)
    updated, energies, scale = pl.pallas_call(
        functools.partial(layer_kernel, shape, basis_count),
        out_shape=(
            jax.ShapeDtypeStruct((chans, atoms), bf16),
            jax.ShapeDtypeStruct((1, atoms), f32),
            jax.ShapeDtypeStruct((1, 128), f32),
        ),
        in_specs=[smem] * 2 + [vmem] * 7,
        out_specs=(vmem,) * 3,
        scratch_shapes=[
            pltpu.VMEM((peers, chans, atoms), bf16),
            pltpu.VMEM((2 * half, peers, chans, width), bf16),
            pltpu.VMEM((2, 3, atoms), f32),
            pltpu.VMEM((2, 1, blocks), i32),
            pltpu.VMEM((2, 2, half), i32),
            pltpu.VMEM((peers, 3, basis_count, chans), f32),
            pltpu.VMEM((peers, 1, chans), f32),
            pltpu.VMEM((2 * blocks, 3, basis_count * width, channels), bf16),
            pltpu.VMEM((2 * blocks, 8, width), f32),
            pltpu.VMEM((3 * blocks, width, width), f32),
            pltpu.VMEM((blocks, width, channels), f32),
            pltpu.VMEM((tiles + 1, 9 * part, channels), f32),
            pltpu.VMEM((channels, blocks * part), bf16),
            pltpu.VMEM((8, blocks * part), f32),
            pltpu.VMEM((peers, chans, blocks * part), bf16),
            pltpu.VMEM((peers, 8, blocks * part), f32),
            pltpu.VMEM((8, 128), f32),
            pltpu.VMEM((groups, 8, 128), f32),
            dma((3,)),
            dma((near,)),
            dma((near,)),
            dma((far,)),
            dma((far,)),
            dma((last,)),
            dma((last,)),
            dma((groups,)),
            dma((groups,)),
        ],
        compiler_params=pltpu.CompilerParams(
            collective_id=0, has_side_effects=True, vmem_limit_bytes=50 * 1024 * 1024
        ),
        name="layer",
    )(
        tile_pairs[0].T,
        tile_count,
        features,
        positions,
        block_counts[None],
        ghost_lists[0],
        radial_w.transpose(1, 0, 2),
        read_w[None],
        mix_w,
    )
    return updated, energies.reshape(-1), scale[0, 0]


def solution(mesh):
    shape = (mesh.shape["atoms"], mesh.shape["chan"])
    in_specs = (
        P("chan", "atoms"),
        P(None, "atoms"),
        P("atoms"),
        P(None, None, "chan"),
        P(),
        P("chan"),
        P("atoms", None, None),
        P("atoms", None, None),
        P("atoms"),
    )
    out_specs = (P("chan", "atoms"), P("atoms"), P())
    return jax.shard_map(
        functools.partial(per_device, shape),
        mesh=mesh,
        in_specs=in_specs,
        out_specs=out_specs,
        check_vma=False,
    )
```

```python
import functools

import jax
import jax.numpy as jnp
from jax import lax
from jax.experimental import pallas as pl
from jax.experimental.pallas import tpu as pltpu
from jax.sharding import PartitionSpec as P

root_three = 3.0**0.5
root_fifteen = 15.0**0.5
half_root_five = 0.5 * 5.0**0.5
half_root_fifteen = 0.5 * 15.0**0.5
cutoff_square = 9.0
soften = 0.25
center_step = 3.0 / 7.0
radial_sharp = 2.0
degrees = ((0,), (1, 2, 3), (4, 5, 6, 7, 8))
MESH = pl.DeviceIdType.MESH
UNROLL = 2


def layer_kernel(
    shape, basis_count, pairs, count, feat_ref, where_ref, present_ref, list_ref, radial_ref,
    read_ref, mix_ref, updated, energies, scale_ref,
    mix, own_in, ghost_in, where_in, present_in, list_in, radial_in, read_in,
    table, spos, rpos, feat_rows, terms, upd, stats, rows_in, stats_in, group_sum, sums_in,
    local_sems, near_s, near_r, far_s, far_r, swap_s, swap_r, last_s, last_r, sums_s, sums_r,
):
    groups, peers = shape
    g, h = lax.axis_index("atoms"), lax.axis_index("chan")
    chans = feat_ref.shape[0]
    blocks = present_ref.shape[1]
    half = list_ref.shape[1]
    width = feat_ref.shape[1] // blocks
    tiles = pairs.shape[1]
    part = width // peers
    after, before = lax.rem(g + 1, groups), lax.rem(g + groups - 1, groups)
    barrier = pltpu.get_barrier_semaphore()

    def signal(device):
        pl.semaphore_signal(barrier, inc=1, device_id=device, device_id_type=MESH)

    for d in range(1, peers):
        to = lax.rem(h + d, peers)
        signal((g, to))

    def greet(d, carry):
        signal((lax.rem(g + d, groups), h))
        return carry

    lax.fori_loop(1, groups, greet, 0)
    locals_ = [
        pltpu.make_async_copy(feat_ref, own_in.at[h], local_sems.at[0]),
        pltpu.make_async_copy(radial_ref, radial_in.at[h], local_sems.at[1]),
        pltpu.make_async_copy(read_ref, read_in.at[h], local_sems.at[2]),
    ]
    mix_copy = pltpu.make_async_copy(mix_ref, mix, local_sems.at[3])
    for copy in locals_:
        copy.start()
    mix_copy.start()
    pl.semaphore_wait(barrier, peers + groups - 2)

    def send(copies, sems, src, dst, device):
        slot = len(copies)
        copy = pltpu.make_async_remote_copy(
            src_ref=src,
            dst_ref=dst,
            send_sem=sems[0].at[slot],
            recv_sem=sems[1].at[slot],
            device_id=device,
            device_id_type=MESH,
        )
        copy.start()
        copies.append(copy)

    near, far, swap, last = [], [], [], []
    for d in range(1, peers):
        to = (g, lax.rem(h + d, peers))
        send(near, (near_s, near_r), feat_ref, own_in.at[h], to)
        send(near, (near_s, near_r), radial_ref, radial_in.at[h], to)
        send(near, (near_s, near_r), read_ref, read_in.at[h], to)
    for n in range(half):
        for side, there in ((0, after), (1, before)):
            block = 2 * n + 1 - side
            send(
                far,
                (far_s, far_r),
                feat_ref.at[:, pl.ds(block * width, width)],
                ghost_in.at[h, side * half + n],
                (there, h),
            )
    for side, there in ((0, after), (1, before)):
        send(far, (far_s, far_r), where_ref, where_in.at[side], (there, h))
        send(far, (far_s, far_r), present_ref, present_in.at[side], (there, h))
        send(far, (far_s, far_r), list_ref, list_in.at[side], (there, h))

    mine = pl.ds(pl.multiple_of(h * part, part), part)
    atom = lax.broadcasted_iota(jnp.int32, (width, 1), 0)
    for b in range(blocks):
        spos[b, 0:3, :] = where_ref[:, b * width : (b + 1) * width]
        for axis in range(3):
            rpos[3 * b + axis] = jnp.broadcast_to(
                where_ref[axis : axis + 1, b * width : (b + 1) * width], (width, width)
            ).T
    diagonal = (
        lax.broadcasted_iota(jnp.int32, (part, width), 0) + h * part
        == lax.broadcasted_iota(jnp.int32, (part, width), 1)
    ).astype(jnp.float32)
    terms[0] = jnp.zeros_like(terms[0])
    for copy in locals_:
        copy.wait()
    for copy in near:
        copy.wait()
    weights = [
        jnp.concatenate([radial_in[n, l] for n in range(peers)], axis=1) for l in range(3)
    ]
    read = jnp.concatenate([read_in[n] for n in range(peers)], axis=1)

    def store_source(code, rows, present):
        masked = jnp.where(atom < present, rows, 0.0)
        for l in range(3):
            for k in range(basis_count):
                table[code, l, k * width : (k + 1) * width, :] = (
                    masked * weights[l][k : k + 1, :]
                ).astype(jnp.bfloat16)

    for b in range(blocks):
        rows = jnp.concatenate(
            [own_in[n, :, b * width : (b + 1) * width] for n in range(peers)], axis=0
        ).astype(jnp.float32).T
        feat_rows[b] = rows
        store_source(b, rows, present_ref[0:1, b : b + 1])

    def one_tile(t, lasts):
        r, q = pairs[0, t], pairs[1, t]
        dx = spos[q, 0:1, :] - rpos[3 * r, mine, :]
        dy = spos[q, 1:2, :] - rpos[3 * r + 1, mine, :]
        dz = spos[q, 2:3, :] - rpos[3 * r + 2, mine, :]
        d2 = dx * dx + dy * dy + dz * dz
        is_self = (r == q).astype(jnp.float32)
        alive = (t < count[0]).astype(jnp.float32)
        edge = jnp.maximum(1.0 - d2 * (1.0 / cutoff_square), 0.0)
        cut = edge * edge * (alive - alive * is_self * diagonal)
        inverse = lax.rsqrt(d2 + soften)
        dist = (d2 + soften) * inverse
        x, y, z = dx * inverse, dy * inverse, dz * inverse
        cx, cy = cut * root_fifteen * x, cut * root_fifteen * y
        cut3 = cut * root_three
        angular = (
            cut,
            cut3 * x,
            cut3 * y,
            cut3 * z,
            cx * y,
            cy * z,
            cut * half_root_five * (2.0 * z * z - x * x - y * y),
            cx * z,
            cut * half_root_fifteen * (x * x - y * y),
        )
        radial = []
        for k in range(basis_count):
            off = dist - center_step * k
            radial.append(jnp.exp(-radial_sharp * off * off))
        previous = lasts[0]
        for b in range(1, blocks):
            previous = jnp.where(r == b, lasts[b], previous)
        for l, ms in enumerate(degrees):
            lhs = jnp.concatenate(
                [
                    jnp.concatenate(
                        [(radial[k] * angular[m]).astype(jnp.bfloat16) for k in range(basis_count)],
                        axis=1,
                    )
                    for m in ms
                ],
                axis=0,
            )
            span = slice(ms[0] * part, (ms[-1] + 1) * part)
            terms[t + 1, span, :] = terms[previous, span, :] + jnp.dot(
                lhs, table[q, l], preferred_element_type=jnp.float32
            )
        return tuple(jnp.where(r == b, t + 1, kept) for b, kept in enumerate(lasts))

    early = blocks // 2
    lasts = lax.fori_loop(0, early, one_tile, (jnp.int32(0),) * blocks, unroll=UNROLL)
    for copy in far:
        copy.wait()
    for d in range(1, peers):
        send(swap, (swap_s, swap_r), ghost_in.at[h], ghost_in.at[h], (g, lax.rem(h + d, peers)))
    lasts = lax.fori_loop(early, blocks, one_tile, lasts, unroll=UNROLL)
    for copy in swap:
        copy.wait()
    for side in range(2):
        for n in range(half):
            listed = list_in[side, 1 - side : 2 - side, n : n + 1]
            code = blocks + side * half + n
            rows, where, present = None, None, None
            for m in range(half):
                block = 2 * m + 1 - side
                new = (
                    jnp.concatenate(
                        [ghost_in[p, side * half + m] for p in range(peers)], axis=0
                    ).astype(jnp.float32),
                    where_in[side, :, block * width : (block + 1) * width],
                    present_in[side, 0:1, block : block + 1],
                )
                if m == 0:
                    rows, where, present = new
                else:
                    is_it = listed == block
                    rows = jnp.where(is_it, new[0], rows)
                    where = jnp.where(is_it, new[1], where)
                    present = jnp.where(is_it, new[2], present)
            store_source(code, rows.T, present)
            spos[code, 0:3, :] = where
    lasts = lax.fori_loop(blocks, tiles, one_tile, lasts, unroll=UNROLL)
    mix_copy.wait()

    basis = [[], [], [], []]
    for b in range(blocks):
        d = [terms[lasts[b], m * part : (m + 1) * part, :] for m in range(9)]
        values = (
            d[0],
            d[0] * d[0],
            d[1] * d[1] + d[2] * d[2] + d[3] * d[3],
            d[4] * d[4] + d[5] * d[5] + d[6] * d[6] + d[7] * d[7] + d[8] * d[8],
        )
        for kept, value in zip(basis, values):
            kept.append(value.astype(jnp.bfloat16))
    mixed = None
    for q in range(4):
        term = jnp.dot(
            jnp.concatenate(basis[q], axis=0), mix[q], preferred_element_type=jnp.float32
        )
        mixed = term if mixed is None else mixed + term
    mixed = mixed / (1.0 + jnp.exp(-mixed))
    feat = jnp.concatenate([feat_rows[b, mine, :] for b in range(blocks)], axis=0)
    my_atom = lax.broadcasted_iota(jnp.int32, (part, 1), 0) + h * part
    present = jnp.concatenate(
        [(my_atom < present_ref[0:1, b : b + 1]).astype(jnp.float32) for b in range(blocks)],
        axis=0,
    )
    hidden = (feat + mixed) * present
    energy = jnp.sum((hidden * read).T, axis=0, keepdims=True)
    square = jnp.sum(energy * energy, axis=1, keepdims=True)
    atoms = jnp.sum(present, axis=0, keepdims=True)
    stats[...] = jnp.concatenate(
        [
            energy,
            jnp.broadcast_to(square, energy.shape),
            jnp.broadcast_to(atoms, energy.shape),
            jnp.zeros((5, energy.shape[1]), jnp.float32),
        ],
        axis=0,
    )
    upd[...] = hidden.T.astype(jnp.bfloat16)
    for d in range(1, peers):
        send(last, (last_s, last_r), stats, stats_in.at[h], (g, lax.rem(h + d, peers)))
    for d in range(1, peers):
        to = lax.rem(h + d, peers)
        send(
            last,
            (last_s, last_r),
            upd.at[pl.ds(pl.multiple_of(to * chans, chans), chans), :],
            rows_in.at[h],
            (g, to),
        )
    stats_in[h] = stats[...]
    rows_in[h] = upd[pl.ds(pl.multiple_of(h * chans, chans), chans), :]
    for copy in last[: peers - 1]:
        copy.wait()
    total = stats_in[0]
    for n in range(1, peers):
        total = total + stats_in[n]
    group_sum[...] = jnp.broadcast_to(total[:, 0:1], group_sum.shape)

    def sum_copy(d):
        return pltpu.make_async_remote_copy(
            src_ref=group_sum,
            dst_ref=sums_in.at[g],
            send_sem=sums_s.at[d],
            recv_sem=sums_r.at[d],
            device_id=(lax.rem(g + d, groups), h),
            device_id_type=MESH,
        )

    def start(d, carry):
        sum_copy(d).start()
        return carry

    lax.fori_loop(1, groups, start, 0)
    sums_in[g] = group_sum[...]
    for copy in last[peers - 1 :]:
        copy.wait()
    pieces = [rows_in[n].astype(jnp.float32) for n in range(peers)]
    for b in range(blocks):
        span = slice(b * part, (b + 1) * part)
        updated[:, b * part * peers : (b + 1) * part * peers] = jnp.concatenate(
            [piece[:, span] for piece in pieces], axis=1
        ).astype(jnp.bfloat16)
    energy = jnp.concatenate(
        [
            stats_in[n][:, b * part : (b + 1) * part]
            for b in range(blocks)
            for n in range(peers)
        ],
        axis=1,
    )[0:1, :]

    def finish(d, carry):
        sum_copy(d).wait()
        return carry

    lax.fori_loop(1, groups, finish, 0)
    whole = jnp.sum(sums_in[...], axis=0)
    scale = jnp.sqrt(1.0 + whole[1:2, :] / whole[2:3, :])
    energies[...] = energy / scale[:, 0:1]
    scale_ref[...] = scale


def per_device(
    shape, features, positions, block_counts, radial_w, mix_w, read_w, ghost_lists, tile_pairs,
    tile_count,
):
    groups, peers = shape
    chans, atoms = features.shape
    blocks = block_counts.shape[0]
    half = ghost_lists.shape[2]
    width = atoms // blocks
    basis_count = radial_w.shape[0]
    channels = mix_w.shape[1]
    tiles = tile_pairs.shape[1]
    part = width // peers
    f32, bf16, i32 = jnp.float32, jnp.bfloat16, jnp.int32
    vmem = pl.BlockSpec(memory_space=pltpu.VMEM)
    smem = pl.BlockSpec(memory_space=pltpu.SMEM)
    hbm = pl.BlockSpec(memory_space=pltpu.HBM)
    dma = pltpu.SemaphoreType.DMA
    near, far, last = 3 * (peers - 1), 2 * half + 6, 2 * (peers - 1)
    updated, energies, scale = pl.pallas_call(
        functools.partial(layer_kernel, shape, basis_count),
        out_shape=(
            jax.ShapeDtypeStruct((chans, atoms), bf16),
            jax.ShapeDtypeStruct((1, atoms), f32),
            jax.ShapeDtypeStruct((1, 128), f32),
        ),
        in_specs=[smem] * 2 + [hbm] + [vmem] * 3 + [hbm, vmem, hbm],
        out_specs=(vmem,) * 3,
        scratch_shapes=[
            pltpu.VMEM(mix_w.shape, bf16),
            pltpu.VMEM((peers, chans, atoms), bf16),
            pltpu.VMEM((peers, 2 * half, chans, width), bf16),
            pltpu.VMEM((2, 3, atoms), f32),
            pltpu.VMEM((2, 1, blocks), i32),
            pltpu.VMEM((2, 2, half), i32),
            pltpu.VMEM((peers, 3, basis_count, chans), f32),
            pltpu.VMEM((peers, 1, chans), f32),
            pltpu.VMEM((2 * blocks, 3, basis_count * width, channels), bf16),
            pltpu.VMEM((2 * blocks, 8, width), f32),
            pltpu.VMEM((3 * blocks, width, width), f32),
            pltpu.VMEM((blocks, width, channels), f32),
            pltpu.VMEM((tiles + 1, 9 * part, channels), f32),
            pltpu.VMEM((channels, blocks * part), bf16),
            pltpu.VMEM((8, blocks * part), f32),
            pltpu.VMEM((peers, chans, blocks * part), bf16),
            pltpu.VMEM((peers, 8, blocks * part), f32),
            pltpu.VMEM((8, 128), f32),
            pltpu.VMEM((groups, 8, 128), f32),
            dma((4,)),
            dma((near,)),
            dma((near,)),
            dma((far,)),
            dma((far,)),
            dma((peers - 1,)),
            dma((peers - 1,)),
            dma((last,)),
            dma((last,)),
            dma((groups,)),
            dma((groups,)),
        ],
        compiler_params=pltpu.CompilerParams(
            collective_id=0, has_side_effects=True, vmem_limit_bytes=50 * 1024 * 1024
        ),
        name="layer",
    )(
        tile_pairs[0].T,
        tile_count,
        features,
        positions,
        block_counts[None],
        ghost_lists[0],
        radial_w.transpose(1, 0, 2),
        read_w[None],
        mix_w,
    )
    return updated, energies.reshape(-1), scale[0, 0]


def solution(mesh):
    shape = (mesh.shape["atoms"], mesh.shape["chan"])
    in_specs = (
        P("chan", "atoms"),
        P(None, "atoms"),
        P("atoms"),
        P(None, None, "chan"),
        P(),
        P("chan"),
        P("atoms", None, None),
        P("atoms", None, None),
        P("atoms"),
    )
    out_specs = (P("chan", "atoms"), P("atoms"), P())
    return jax.shard_map(
        functools.partial(per_device, shape),
        mesh=mesh,
        in_specs=in_specs,
        out_specs=out_specs,
        check_vma=False,
    )
```

```python
import functools

import jax
import jax.numpy as jnp
from jax import lax
from jax.experimental import pallas as pl
from jax.experimental.pallas import tpu as pltpu
from jax.sharding import PartitionSpec as P

root_three = 3.0**0.5
root_fifteen = 15.0**0.5
half_root_five = 0.5 * 5.0**0.5
half_root_fifteen = 0.5 * 15.0**0.5
cutoff_square = 9.0
soften = 0.25
center_step = 3.0 / 7.0
radial_sharp = 2.0
degrees = ((0,), (1, 2, 3), (4, 5, 6, 7, 8))
MESH = pl.DeviceIdType.MESH
UNROLL = 2


def layer_kernel(
    shape, basis_count, pairs_ref, count_ref, feat_ref, where_hbm, present_hbm, list_ref, radial_ref,
    read_ref, mix_ref, updated, energies, scale_ref,
    pairs, count, where_ref, present_ref, mix, own_in, ghost_in, where_in, present_in, list_in, radial_in, read_in,
    table, spos, rpos, feat_rows, terms, upd, stats, rows_in, stats_in, group_sum, sums_in,
    local_sems, near_s, near_r, far_s, far_r, swap_s, swap_r, last_s, last_r, sums_s, sums_r,
):
    groups, peers = shape
    g, h = lax.axis_index("atoms"), lax.axis_index("chan")
    chans = feat_ref.shape[0]
    blocks = present_ref.shape[1]
    half = list_ref.shape[1]
    width = feat_ref.shape[1] // blocks
    tiles = pairs.shape[1]
    part = width // peers
    after, before = lax.rem(g + 1, groups), lax.rem(g + groups - 1, groups)
    barrier = pltpu.get_barrier_semaphore()

    def signal(device):
        pl.semaphore_signal(barrier, inc=1, device_id=device, device_id_type=MESH)

    for d in range(1, peers):
        to = lax.rem(h + d, peers)
        signal((g, to))

    def greet(d, carry):
        signal((lax.rem(g + d, groups), h))
        return carry

    lax.fori_loop(1, groups, greet, 0)
    locals_ = [
        pltpu.make_async_copy(feat_ref, own_in.at[h], local_sems.at[0]),
        pltpu.make_async_copy(radial_ref, radial_in.at[h], local_sems.at[1]),
        pltpu.make_async_copy(read_ref, read_in.at[h], local_sems.at[2]),
    ]
    mix_copy = pltpu.make_async_copy(mix_ref, mix, local_sems.at[3])
    for copy in locals_:
        copy.start()
    mix_copy.start()
    small = [
        pltpu.make_async_copy(where_hbm, where_ref, local_sems.at[4]),
        pltpu.make_async_copy(present_hbm, present_ref, local_sems.at[5]),
        pltpu.make_async_copy(pairs_ref, pairs, local_sems.at[6]),
        pltpu.make_async_copy(count_ref, count, local_sems.at[7]),
    ]
    for copy in small:
        copy.start()
    pl.semaphore_wait(barrier, peers + groups - 2)

    def send(copies, sems, src, dst, device):
        slot = len(copies)
        copy = pltpu.make_async_remote_copy(
            src_ref=src,
            dst_ref=dst,
            send_sem=sems[0].at[slot],
            recv_sem=sems[1].at[slot],
            device_id=device,
            device_id_type=MESH,
        )
        copy.start()
        copies.append(copy)

    near, far, swap, last = [], [], [], []
    for d in range(1, peers):
        to = (g, lax.rem(h + d, peers))
        send(near, (near_s, near_r), feat_ref, own_in.at[h], to)
        send(near, (near_s, near_r), radial_ref, radial_in.at[h], to)
        send(near, (near_s, near_r), read_ref, read_in.at[h], to)
    for n in range(half):
        for side, there in ((0, after), (1, before)):
            block = 2 * n + 1 - side
            send(
                far,
                (far_s, far_r),
                feat_ref.at[:, pl.ds(block * width, width)],
                ghost_in.at[h, side * half + n],
                (there, h),
            )
    for side, there in ((0, after), (1, before)):
        send(far, (far_s, far_r), where_hbm, where_in.at[side], (there, h))
        send(far, (far_s, far_r), present_hbm, present_in.at[side], (there, h))
        send(far, (far_s, far_r), list_ref, list_in.at[side], (there, h))

    for copy in small:
        copy.wait()
    mine = pl.ds(pl.multiple_of(h * part, part), part)
    atom = lax.broadcasted_iota(jnp.int32, (width, 1), 0)
    for b in range(blocks):
        spos[b, 0:3, :] = where_ref[:, b * width : (b + 1) * width]
        for axis in range(3):
            rpos[3 * b + axis] = jnp.broadcast_to(
                where_ref[axis : axis + 1, b * width : (b + 1) * width], (width, width)
            ).T
    diagonal = (
        lax.broadcasted_iota(jnp.int32, (part, width), 0) + h * part
        == lax.broadcasted_iota(jnp.int32, (part, width), 1)
    ).astype(jnp.float32)
    terms[0] = jnp.zeros_like(terms[0])
    for copy in locals_:
        copy.wait()
    for copy in near:
        copy.wait()
    weights = [
        jnp.concatenate([radial_in[n, l] for n in range(peers)], axis=1) for l in range(3)
    ]
    read = jnp.concatenate([read_in[n] for n in range(peers)], axis=1)

    def store_source(code, rows, present):
        masked = jnp.where(atom < present, rows, 0.0)
        for l in range(3):
            for k in range(basis_count):
                table[code, l, k * width : (k + 1) * width, :] = (
                    masked * weights[l][k : k + 1, :]
                ).astype(jnp.bfloat16)

    for b in range(blocks):
        rows = jnp.concatenate(
            [own_in[n, :, b * width : (b + 1) * width] for n in range(peers)], axis=0
        ).astype(jnp.float32).T
        feat_rows[b] = rows
        store_source(b, rows, present_ref[0:1, b : b + 1])

    def one_tile(t, lasts):
        r, q = pairs[0, t], pairs[1, t]
        dx = spos[q, 0:1, :] - rpos[3 * r, mine, :]
        dy = spos[q, 1:2, :] - rpos[3 * r + 1, mine, :]
        dz = spos[q, 2:3, :] - rpos[3 * r + 2, mine, :]
        d2 = dx * dx + dy * dy + dz * dz
        is_self = (r == q).astype(jnp.float32)
        alive = (t < count[0]).astype(jnp.float32)
        edge = jnp.maximum(1.0 - d2 * (1.0 / cutoff_square), 0.0)
        cut = edge * edge * (alive - alive * is_self * diagonal)
        inverse = lax.rsqrt(d2 + soften)
        dist = (d2 + soften) * inverse
        x, y, z = dx * inverse, dy * inverse, dz * inverse
        cx, cy = cut * root_fifteen * x, cut * root_fifteen * y
        cut3 = cut * root_three
        angular = (
            cut,
            cut3 * x,
            cut3 * y,
            cut3 * z,
            cx * y,
            cy * z,
            cut * half_root_five * (2.0 * z * z - x * x - y * y),
            cx * z,
            cut * half_root_fifteen * (x * x - y * y),
        )
        radial = []
        for k in range(basis_count):
            off = dist - center_step * k
            radial.append(jnp.exp(-radial_sharp * off * off))
        previous = lasts[0]
        for b in range(1, blocks):
            previous = jnp.where(r == b, lasts[b], previous)
        for l, ms in enumerate(degrees):
            lhs = jnp.concatenate(
                [
                    jnp.concatenate(
                        [(radial[k] * angular[m]).astype(jnp.bfloat16) for k in range(basis_count)],
                        axis=1,
                    )
                    for m in ms
                ],
                axis=0,
            )
            span = slice(ms[0] * part, (ms[-1] + 1) * part)
            terms[t + 1, span, :] = terms[previous, span, :] + jnp.dot(
                lhs, table[q, l], preferred_element_type=jnp.float32
            )
        return tuple(jnp.where(r == b, t + 1, kept) for b, kept in enumerate(lasts))

    early = blocks // 2
    lasts = lax.fori_loop(0, early, one_tile, (jnp.int32(0),) * blocks, unroll=UNROLL)
    for copy in far:
        copy.wait()
    for d in range(1, peers):
        send(swap, (swap_s, swap_r), ghost_in.at[h], ghost_in.at[h], (g, lax.rem(h + d, peers)))
    lasts = lax.fori_loop(early, blocks, one_tile, lasts, unroll=UNROLL)
    for copy in swap:
        copy.wait()
    for side in range(2):
        for n in range(half):
            listed = list_in[side, 1 - side : 2 - side, n : n + 1]
            code = blocks + side * half + n
            rows, where, present = None, None, None
            for m in range(half):
                block = 2 * m + 1 - side
                new = (
                    jnp.concatenate(
                        [ghost_in[p, side * half + m] for p in range(peers)], axis=0
                    ).astype(jnp.float32),
                    where_in[side, :, block * width : (block + 1) * width],
                    present_in[side, 0:1, block : block + 1],
                )
                if m == 0:
                    rows, where, present = new
                else:
                    is_it = listed == block
                    rows = jnp.where(is_it, new[0], rows)
                    where = jnp.where(is_it, new[1], where)
                    present = jnp.where(is_it, new[2], present)
            store_source(code, rows.T, present)
            spos[code, 0:3, :] = where
    lasts = lax.fori_loop(blocks, tiles, one_tile, lasts, unroll=UNROLL)
    mix_copy.wait()

    basis = [[], [], [], []]
    for b in range(blocks):
        d = [terms[lasts[b], m * part : (m + 1) * part, :] for m in range(9)]
        values = (
            d[0],
            d[0] * d[0],
            d[1] * d[1] + d[2] * d[2] + d[3] * d[3],
            d[4] * d[4] + d[5] * d[5] + d[6] * d[6] + d[7] * d[7] + d[8] * d[8],
        )
        for kept, value in zip(basis, values):
            kept.append(value.astype(jnp.bfloat16))
    mixed = None
    for q in range(4):
        term = jnp.dot(
            jnp.concatenate(basis[q], axis=0), mix[q], preferred_element_type=jnp.float32
        )
        mixed = term if mixed is None else mixed + term
    mixed = mixed / (1.0 + jnp.exp(-mixed))
    feat = jnp.concatenate([feat_rows[b, mine, :] for b in range(blocks)], axis=0)
    my_atom = lax.broadcasted_iota(jnp.int32, (part, 1), 0) + h * part
    present = jnp.concatenate(
        [(my_atom < present_ref[0:1, b : b + 1]).astype(jnp.float32) for b in range(blocks)],
        axis=0,
    )
    hidden = (feat + mixed) * present
    energy = jnp.sum((hidden * read).T, axis=0, keepdims=True)
    square = jnp.sum(energy * energy, axis=1, keepdims=True)
    atoms = jnp.sum(present, axis=0, keepdims=True)
    stats[...] = jnp.concatenate(
        [
            energy,
            jnp.broadcast_to(square, energy.shape),
            jnp.broadcast_to(atoms, energy.shape),
            jnp.zeros((5, energy.shape[1]), jnp.float32),
        ],
        axis=0,
    )
    upd[...] = hidden.T.astype(jnp.bfloat16)
    for d in range(1, peers):
        send(last, (last_s, last_r), stats, stats_in.at[h], (g, lax.rem(h + d, peers)))
    for d in range(1, peers):
        to = lax.rem(h + d, peers)
        send(
            last,
            (last_s, last_r),
            upd.at[pl.ds(pl.multiple_of(to * chans, chans), chans), :],
            rows_in.at[h],
            (g, to),
        )
    stats_in[h] = stats[...]
    rows_in[h] = upd[pl.ds(pl.multiple_of(h * chans, chans), chans), :]
    for copy in last[: peers - 1]:
        copy.wait()
    total = stats_in[0]
    for n in range(1, peers):
        total = total + stats_in[n]
    group_sum[...] = jnp.broadcast_to(total[:, 0:1], group_sum.shape)

    def sum_copy(d):
        return pltpu.make_async_remote_copy(
            src_ref=group_sum,
            dst_ref=sums_in.at[g],
            send_sem=sums_s.at[d],
            recv_sem=sums_r.at[d],
            device_id=(lax.rem(g + d, groups), h),
            device_id_type=MESH,
        )

    def start(d, carry):
        sum_copy(d).start()
        return carry

    lax.fori_loop(1, groups, start, 0)
    sums_in[g] = group_sum[...]
    for copy in last[peers - 1 :]:
        copy.wait()
    pieces = [rows_in[n].astype(jnp.float32) for n in range(peers)]
    for b in range(blocks):
        span = slice(b * part, (b + 1) * part)
        updated[:, b * part * peers : (b + 1) * part * peers] = jnp.concatenate(
            [piece[:, span] for piece in pieces], axis=1
        ).astype(jnp.bfloat16)
    energy = jnp.concatenate(
        [
            stats_in[n][:, b * part : (b + 1) * part]
            for b in range(blocks)
            for n in range(peers)
        ],
        axis=1,
    )[0:1, :]

    def finish(d, carry):
        sum_copy(d).wait()
        return carry

    lax.fori_loop(1, groups, finish, 0)
    whole = jnp.sum(sums_in[...], axis=0)
    scale = jnp.sqrt(1.0 + whole[1:2, :] / whole[2:3, :])
    energies[...] = energy / scale[:, 0:1]
    scale_ref[...] = scale


def per_device(
    shape, features, positions, block_counts, radial_w, mix_w, read_w, ghost_lists, tile_pairs,
    tile_count,
):
    groups, peers = shape
    chans, atoms = features.shape
    blocks = block_counts.shape[0]
    half = ghost_lists.shape[2]
    width = atoms // blocks
    basis_count = radial_w.shape[0]
    channels = mix_w.shape[1]
    tiles = tile_pairs.shape[1]
    part = width // peers
    f32, bf16, i32 = jnp.float32, jnp.bfloat16, jnp.int32
    vmem = pl.BlockSpec(memory_space=pltpu.VMEM)
    hbm = pl.BlockSpec(memory_space=pltpu.HBM)
    dma = pltpu.SemaphoreType.DMA
    near, far, last = 3 * (peers - 1), 2 * half + 6, 2 * (peers - 1)
    updated, energies, scale = pl.pallas_call(
        functools.partial(layer_kernel, shape, basis_count),
        out_shape=(
            jax.ShapeDtypeStruct((chans, atoms), bf16),
            jax.ShapeDtypeStruct((1, atoms), f32),
            jax.ShapeDtypeStruct((1, 128), f32),
        ),
        in_specs=[hbm] * 9,
        out_specs=(vmem,) * 3,
        scratch_shapes=[
            pltpu.SMEM((2, tiles), i32),
            pltpu.SMEM((1,), i32),
            pltpu.VMEM((3, atoms), f32),
            pltpu.VMEM((1, blocks), i32),
            pltpu.VMEM(mix_w.shape, bf16),
            pltpu.VMEM((peers, chans, atoms), bf16),
            pltpu.VMEM((peers, 2 * half, chans, width), bf16),
            pltpu.VMEM((2, 3, atoms), f32),
            pltpu.VMEM((2, 1, blocks), i32),
            pltpu.VMEM((2, 2, half), i32),
            pltpu.VMEM((peers, 3, basis_count, chans), f32),
            pltpu.VMEM((peers, 1, chans), f32),
            pltpu.VMEM((2 * blocks, 3, basis_count * width, channels), bf16),
            pltpu.VMEM((2 * blocks, 8, width), f32),
            pltpu.VMEM((3 * blocks, width, width), f32),
            pltpu.VMEM((blocks, width, channels), f32),
            pltpu.VMEM((tiles + 1, 9 * part, channels), f32),
            pltpu.VMEM((channels, blocks * part), bf16),
            pltpu.VMEM((8, blocks * part), f32),
            pltpu.VMEM((peers, chans, blocks * part), bf16),
            pltpu.VMEM((peers, 8, blocks * part), f32),
            pltpu.VMEM((8, 128), f32),
            pltpu.VMEM((groups, 8, 128), f32),
            dma((8,)),
            dma((near,)),
            dma((near,)),
            dma((far,)),
            dma((far,)),
            dma((peers - 1,)),
            dma((peers - 1,)),
            dma((last,)),
            dma((last,)),
            dma((groups,)),
            dma((groups,)),
        ],
        compiler_params=pltpu.CompilerParams(
            collective_id=0, has_side_effects=True, vmem_limit_bytes=66860000
        ),
        name="layer",
    )(
        tile_pairs[0].T,
        tile_count,
        features,
        positions,
        block_counts[None],
        ghost_lists[0],
        radial_w.transpose(1, 0, 2),
        read_w[None],
        mix_w,
    )
    return updated, energies.reshape(-1), scale[0, 0]


def solution(mesh):
    shape = (mesh.shape["atoms"], mesh.shape["chan"])
    in_specs = (
        P("chan", "atoms"),
        P(None, "atoms"),
        P("atoms"),
        P(None, None, "chan"),
        P(),
        P("chan"),
        P("atoms", None, None),
        P("atoms", None, None),
        P("atoms"),
    )
    out_specs = (P("chan", "atoms"), P("atoms"), P())
    return jax.shard_map(
        functools.partial(per_device, shape),
        mesh=mesh,
        in_specs=in_specs,
        out_specs=out_specs,
        check_vma=False,
    )
```

```python
import functools

import jax
import jax.numpy as jnp
from jax import lax
from jax.experimental import pallas as pl
from jax.experimental.pallas import tpu as pltpu
from jax.sharding import PartitionSpec as P

root_three = 3.0**0.5
root_fifteen = 15.0**0.5
half_root_five = 0.5 * 5.0**0.5
half_root_fifteen = 0.5 * 15.0**0.5
cutoff_square = 9.0
soften = 0.25
center_step = 3.0 / 7.0
radial_sharp = 2.0
degrees = ((0,), (1, 2, 3), (4, 5, 6, 7, 8))
MESH = pl.DeviceIdType.MESH
UNROLL = 2


def layer_kernel(
    shape, basis_count, pairs_ref, count_ref, feat_ref, where_hbm, present_hbm, list_ref, radial_ref,
    read_ref, mix_ref, updated, energies, scale_ref,
    pairs, count, where_ref, present_ref, mix, own_in, ghost_in, where_in, present_in, list_in, radial_in, read_in,
    table, spos, rpos, feat_rows, terms, upd, stats, rows_in, stats_in, group_sum, sums_in,
    local_sems, near_s, near_r, far_s, far_r, swap_s, swap_r, last_s, last_r, sums_s, sums_r,
):
    groups, peers = shape
    g, h = lax.axis_index("atoms"), lax.axis_index("chan")
    chans = feat_ref.shape[0]
    blocks = present_ref.shape[1]
    half = list_ref.shape[1]
    width = feat_ref.shape[1] // blocks
    tiles = pairs.shape[1]
    part = width // peers
    after, before = lax.rem(g + 1, groups), lax.rem(g + groups - 1, groups)
    barrier = pltpu.get_barrier_semaphore()

    def signal(device):
        pl.semaphore_signal(barrier, inc=1, device_id=device, device_id_type=MESH)

    for d in range(1, peers):
        to = lax.rem(h + d, peers)
        signal((g, to))

    def greet(d, carry):
        signal((lax.rem(g + d, groups), h))
        return carry

    lax.fori_loop(1, groups, greet, 0)
    locals_ = [
        pltpu.make_async_copy(feat_ref, own_in.at[h], local_sems.at[0]),
        pltpu.make_async_copy(radial_ref, radial_in.at[h], local_sems.at[1]),
        pltpu.make_async_copy(read_ref, read_in.at[h], local_sems.at[2]),
    ]
    mix_copy = pltpu.make_async_copy(mix_ref, mix, local_sems.at[3])
    for copy in locals_:
        copy.start()
    mix_copy.start()
    small = [
        pltpu.make_async_copy(where_hbm, where_ref, local_sems.at[4]),
        pltpu.make_async_copy(present_hbm, present_ref, local_sems.at[5]),
        pltpu.make_async_copy(pairs_ref, pairs, local_sems.at[6]),
        pltpu.make_async_copy(count_ref, count, local_sems.at[7]),
    ]
    for copy in small:
        copy.start()
    pl.semaphore_wait(barrier, peers + groups - 2)

    def send(copies, sems, src, dst, device):
        slot = len(copies)
        copy = pltpu.make_async_remote_copy(
            src_ref=src,
            dst_ref=dst,
            send_sem=sems[0].at[slot],
            recv_sem=sems[1].at[slot],
            device_id=device,
            device_id_type=MESH,
        )
        copy.start()
        copies.append(copy)

    near, far, swap, last = [], [], [], []
    for d in range(1, peers):
        to = (g, lax.rem(h + d, peers))
        send(near, (near_s, near_r), feat_ref, own_in.at[h], to)
        send(near, (near_s, near_r), radial_ref, radial_in.at[h], to)
        send(near, (near_s, near_r), read_ref, read_in.at[h], to)
    for n in range(half):
        for side, there in ((0, after), (1, before)):
            block = 2 * n + 1 - side
            send(
                far,
                (far_s, far_r),
                feat_ref.at[:, pl.ds(block * width, width)],
                ghost_in.at[h, side * half + n],
                (there, h),
            )
    for side, there in ((0, after), (1, before)):
        send(far, (far_s, far_r), where_hbm, where_in.at[side], (there, h))
        send(far, (far_s, far_r), present_hbm, present_in.at[side], (there, h))
        send(far, (far_s, far_r), list_ref, list_in.at[side], (there, h))

    for copy in small:
        copy.wait()
    mine = pl.ds(pl.multiple_of(h * part, part), part)
    atom = lax.broadcasted_iota(jnp.int32, (width, 1), 0)
    for b in range(blocks):
        spos[b, 0:3, :] = where_ref[:, b * width : (b + 1) * width]
        for axis in range(3):
            rpos[3 * b + axis] = jnp.broadcast_to(
                where_ref[axis : axis + 1, b * width : (b + 1) * width], (width, width)
            ).T
    diagonal = (
        lax.broadcasted_iota(jnp.int32, (part, width), 0) + h * part
        == lax.broadcasted_iota(jnp.int32, (part, width), 1)
    ).astype(jnp.float32)
    terms[0] = jnp.zeros_like(terms[0])
    for copy in locals_:
        copy.wait()
    for copy in near:
        copy.wait()
    weights = [
        jnp.concatenate([radial_in[n, l] for n in range(peers)], axis=1) for l in range(3)
    ]
    read = jnp.concatenate([read_in[n] for n in range(peers)], axis=1)

    def store_source(code, rows, present):
        masked = jnp.where(atom < present, rows, 0.0)
        for l in range(3):
            for k in range(basis_count):
                table[code, l, k * width : (k + 1) * width, :] = (
                    masked * weights[l][k : k + 1, :]
                ).astype(jnp.bfloat16)

    for b in range(blocks):
        rows = jnp.concatenate(
            [own_in[n, :, b * width : (b + 1) * width] for n in range(peers)], axis=0
        ).astype(jnp.float32).T
        feat_rows[b] = rows
        store_source(b, rows, present_ref[0:1, b : b + 1])

    def one_tile(t, lasts):
        r, q = pairs[0, t], pairs[1, t]
        dx = spos[q, 0:1, :] - rpos[3 * r, mine, :]
        dy = spos[q, 1:2, :] - rpos[3 * r + 1, mine, :]
        dz = spos[q, 2:3, :] - rpos[3 * r + 2, mine, :]
        d2 = dx * dx + dy * dy + dz * dz
        is_self = (r == q).astype(jnp.float32)
        alive = (t < count[0]).astype(jnp.float32)
        edge = jnp.maximum(1.0 - d2 * (1.0 / cutoff_square), 0.0)
        cut = edge * edge * (alive - alive * is_self * diagonal)
        inverse = lax.rsqrt(d2 + soften)
        dist = (d2 + soften) * inverse
        x, y, z = dx * inverse, dy * inverse, dz * inverse
        cx, cy = cut * root_fifteen * x, cut * root_fifteen * y
        cut3 = cut * root_three
        angular = (
            cut,
            cut3 * x,
            cut3 * y,
            cut3 * z,
            cx * y,
            cy * z,
            cut * half_root_five * (2.0 * z * z - x * x - y * y),
            cx * z,
            cut * half_root_fifteen * (x * x - y * y),
        )
        radial = []
        for k in range(basis_count):
            off = dist - center_step * k
            radial.append(jnp.exp(-radial_sharp * off * off))
        previous = lasts[0]
        for b in range(1, blocks):
            previous = jnp.where(r == b, lasts[b], previous)
        for l, ms in enumerate(degrees):
            lhs = jnp.concatenate(
                [
                    jnp.concatenate(
                        [(radial[k] * angular[m]).astype(jnp.bfloat16) for k in range(basis_count)],
                        axis=1,
                    )
                    for m in ms
                ],
                axis=0,
            )
            span = slice(ms[0] * part, (ms[-1] + 1) * part)
            terms[t + 1, span, :] = terms[previous, span, :] + jnp.dot(
                lhs, table[q, l], preferred_element_type=jnp.float32
            )
        return tuple(jnp.where(r == b, t + 1, kept) for b, kept in enumerate(lasts))

    early = blocks // 2
    lasts = lax.fori_loop(0, early, one_tile, (jnp.int32(0),) * blocks, unroll=UNROLL)
    for copy in far:
        copy.wait()
    for d in range(1, peers):
        send(swap, (swap_s, swap_r), ghost_in.at[h], ghost_in.at[h], (g, lax.rem(h + d, peers)))
    lasts = lax.fori_loop(early, blocks, one_tile, lasts, unroll=UNROLL)
    for copy in swap:
        copy.wait()
    for side in range(2):
        for n in range(half):
            listed = list_in[side, 1 - side : 2 - side, n : n + 1]
            code = blocks + side * half + n
            rows, where, present = None, None, None
            for m in range(half):
                block = 2 * m + 1 - side
                new = (
                    jnp.concatenate(
                        [ghost_in[p, side * half + m] for p in range(peers)], axis=0
                    ).astype(jnp.float32),
                    where_in[side, :, block * width : (block + 1) * width],
                    present_in[side, 0:1, block : block + 1],
                )
                if m == 0:
                    rows, where, present = new
                else:
                    is_it = listed == block
                    rows = jnp.where(is_it, new[0], rows)
                    where = jnp.where(is_it, new[1], where)
                    present = jnp.where(is_it, new[2], present)
            store_source(code, rows.T, present)
            spos[code, 0:3, :] = where
    lasts = lax.fori_loop(blocks, tiles, one_tile, lasts, unroll=UNROLL)
    mix_copy.wait()

    basis = [[], [], [], []]
    for b in range(blocks):
        d = [terms[lasts[b], m * part : (m + 1) * part, :] for m in range(9)]
        values = (
            d[0],
            d[0] * d[0],
            d[1] * d[1] + d[2] * d[2] + d[3] * d[3],
            d[4] * d[4] + d[5] * d[5] + d[6] * d[6] + d[7] * d[7] + d[8] * d[8],
        )
        for kept, value in zip(basis, values):
            kept.append(value.astype(jnp.bfloat16))
    mixed = None
    for q in range(4):
        term = jnp.dot(
            jnp.concatenate(basis[q], axis=0), mix[q], preferred_element_type=jnp.float32
        )
        mixed = term if mixed is None else mixed + term
    mixed = mixed / (1.0 + jnp.exp(-mixed))
    feat = jnp.concatenate([feat_rows[b, mine, :] for b in range(blocks)], axis=0)
    my_atom = lax.broadcasted_iota(jnp.int32, (part, 1), 0) + h * part
    present = jnp.concatenate(
        [(my_atom < present_ref[0:1, b : b + 1]).astype(jnp.float32) for b in range(blocks)],
        axis=0,
    )
    hidden = (feat + mixed) * present
    energy = jnp.sum((hidden * read).T, axis=0, keepdims=True)
    square = jnp.sum(energy * energy, axis=1, keepdims=True)
    atoms = jnp.sum(present, axis=0, keepdims=True)
    stats[...] = jnp.concatenate(
        [
            energy,
            jnp.broadcast_to(square, energy.shape),
            jnp.broadcast_to(atoms, energy.shape),
            jnp.zeros((5, energy.shape[1]), jnp.float32),
        ],
        axis=0,
    )
    upd[...] = hidden.T.astype(jnp.bfloat16)
    for d in range(1, peers):
        send(last, (last_s, last_r), stats, stats_in.at[h], (g, lax.rem(h + d, peers)))
    for d in range(1, peers):
        to = lax.rem(h + d, peers)
        send(
            last,
            (last_s, last_r),
            upd.at[pl.ds(pl.multiple_of(to * chans, chans), chans), :],
            rows_in.at[h],
            (g, to),
        )
    stats_in[h] = stats[...]
    rows_in[h] = upd[pl.ds(pl.multiple_of(h * chans, chans), chans), :]
    for copy in last[: peers - 1]:
        copy.wait()
    total = stats_in[0]
    for n in range(1, peers):
        total = total + stats_in[n]
    group_sum[...] = jnp.broadcast_to(total[:, 0:1], group_sum.shape)

    def sum_copy(d):
        return pltpu.make_async_remote_copy(
            src_ref=group_sum,
            dst_ref=sums_in.at[g],
            send_sem=sums_s.at[d],
            recv_sem=sums_r.at[d],
            device_id=(lax.rem(g + d, groups), h),
            device_id_type=MESH,
        )

    def start(d, carry):
        sum_copy(d).start()
        return carry

    lax.fori_loop(1, groups, start, 0)
    sums_in[g] = group_sum[...]
    for copy in last[peers - 1 :]:
        copy.wait()
    pieces = [rows_in[n].astype(jnp.float32) for n in range(peers)]
    for b in range(blocks):
        span = slice(b * part, (b + 1) * part)
        updated[:, b * part * peers : (b + 1) * part * peers] = jnp.concatenate(
            [piece[:, span] for piece in pieces], axis=1
        ).astype(jnp.bfloat16)
    energy = jnp.concatenate(
        [
            stats_in[n][:, b * part : (b + 1) * part]
            for b in range(blocks)
            for n in range(peers)
        ],
        axis=1,
    )[0:1, :]

    def finish(d, carry):
        sum_copy(d).wait()
        return carry

    lax.fori_loop(1, groups, finish, 0)
    whole = jnp.sum(sums_in[...], axis=0)
    scale = jnp.sqrt(1.0 + whole[1:2, :] / whole[2:3, :])
    energies[...] = energy / scale[:, 0:1]
    scale_ref[...] = scale


def per_device(
    shape, features, positions, block_counts, radial_w, mix_w, read_w, ghost_lists, tile_pairs,
    tile_count,
):
    groups, peers = shape
    chans, atoms = features.shape
    blocks = block_counts.shape[0]
    half = ghost_lists.shape[2]
    width = atoms // blocks
    basis_count = radial_w.shape[0]
    channels = mix_w.shape[1]
    tiles = tile_pairs.shape[1]
    part = width // peers
    f32, bf16, i32 = jnp.float32, jnp.bfloat16, jnp.int32
    vmem = pl.BlockSpec(memory_space=pltpu.VMEM)
    hbm = pl.BlockSpec(memory_space=pltpu.HBM)
    dma = pltpu.SemaphoreType.DMA
    near, far, last = 3 * (peers - 1), 2 * half + 6, 2 * (peers - 1)
    updated, energies, scale = pl.pallas_call(
        functools.partial(layer_kernel, shape, basis_count),
        out_shape=(
            jax.ShapeDtypeStruct((chans, atoms), bf16),
            jax.ShapeDtypeStruct((1, atoms), f32),
            jax.ShapeDtypeStruct((1, 128), f32),
        ),
        in_specs=[hbm] * 9,
        out_specs=(vmem,) * 3,
        scratch_shapes=[
            pltpu.SMEM((2, tiles), i32),
            pltpu.SMEM((1,), i32),
            pltpu.VMEM((3, atoms), f32),
            pltpu.VMEM((1, blocks), i32),
            pltpu.VMEM(mix_w.shape, bf16),
            pltpu.VMEM((peers, chans, atoms), bf16),
            pltpu.VMEM((peers, 2 * half, chans, width), bf16),
            pltpu.VMEM((2, 3, atoms), f32),
            pltpu.VMEM((2, 1, blocks), i32),
            pltpu.VMEM((2, 2, half), i32),
            pltpu.VMEM((peers, 3, basis_count, chans), f32),
            pltpu.VMEM((peers, 1, chans), f32),
            pltpu.VMEM((2 * blocks, 3, basis_count * width, channels), bf16),
            pltpu.VMEM((2 * blocks, 8, width), f32),
            pltpu.VMEM((3 * blocks, width, width), f32),
            pltpu.VMEM((blocks, width, channels), f32),
            pltpu.VMEM((tiles + 1, 9 * part, channels), f32),
            pltpu.VMEM((channels, blocks * part), bf16),
            pltpu.VMEM((8, blocks * part), f32),
            pltpu.VMEM((peers, chans, blocks * part), bf16),
            pltpu.VMEM((peers, 8, blocks * part), f32),
            pltpu.VMEM((8, 128), f32),
            pltpu.VMEM((groups, 8, 128), f32),
            dma((8,)),
            dma((near,)),
            dma((near,)),
            dma((far,)),
            dma((far,)),
            dma((peers - 1,)),
            dma((peers - 1,)),
            dma((last,)),
            dma((last,)),
            dma((groups,)),
            dma((groups,)),
        ],
        compiler_params=pltpu.CompilerParams(
            collective_id=0, has_side_effects=True, vmem_limit_bytes=50 * 1024 * 1024
        ),
        name="layer",
    )(
        pltpu.with_memory_space_constraint(tile_pairs[0].T, pltpu.HBM),
        tile_count,
        *(
            pltpu.with_memory_space_constraint(value, pltpu.HBM)
            for value in (
                features,
                positions,
                block_counts[None],
                ghost_lists[0],
                radial_w.transpose(1, 0, 2),
                read_w[None],
                mix_w,
            )
        )
    )
    return updated, energies.reshape(-1), scale[0, 0]


def solution(mesh):
    shape = (mesh.shape["atoms"], mesh.shape["chan"])
    in_specs = (
        P("chan", "atoms"),
        P(None, "atoms"),
        P("atoms"),
        P(None, None, "chan"),
        P(),
        P("chan"),
        P("atoms", None, None),
        P("atoms", None, None),
        P("atoms"),
    )
    out_specs = (P("chan", "atoms"), P("atoms"), P())
    return jax.shard_map(
        functools.partial(per_device, shape),
        mesh=mesh,
        in_specs=in_specs,
        out_specs=out_specs,
        check_vma=False,
    )
```
